32 devices in a mesh: rep: 4 (over y, x), zero: 8 (over z, core).
Axes of the slice: x: 2, y: 2, z: 4, core: 2. Of those that a mesh axis runs over, the one named last changes fastest.
Arguments:
- pre_norm: bfloat16 [512, 8192], P(('rep', 'zero')), may hold values from -6 to 6
- upstream: bfloat16 [512, 8192], P(('rep', 'zero')), may hold values from -20 to 20
- norm_gain: float32 [8192], replicated, may hold values from 0.1 to 1.9
- saved_mean: float32 [8192], replicated, may hold values from -4 to 4
- inv_std: float32 [8192], replicated, may hold values from 0.5 to 1.5
- features: bfloat16 [25088, 512], P(('rep', 'zero')), may hold values from -6 to 6
- out_grads: bfloat16 [25088, 2048], P(('rep', 'zero')), may hold values from -24 to 24
Outputs:
- input_grad: bfloat16 [512, 8192], P(('rep', 'zero'))
- gain_grad: float32 [8192], replicated
- bias_grad: float32 [8192], replicated
- weight_grad: float32 [512, 2048], P('zero')
The draws below stay inside these ranges and needn't reach their ends.
All inputs are finite; a program needn't handle non-finite values.
Results may differ from the reference program's by a relative error of at most 0.001.
Values sent between devices are 32-bit elements; how exact they have to be, the bound alone decides.
No kernel may reach another device: no remote copies, remote signals or barrier semaphores. Data moves between devices by JAX's collectives and lax.ppermute only.
A program may use at most 64 MiB of HBM per device.

```python
import math
import jax
import jax.numpy as jnp
from jax import lax

F = 8192
CIN = 512
COUT = 2048
SPATIAL = 49
IMG_DEV = 16
IMAGES = 512


def draw_upstream(key, part):
    key_noise, key_offset, key_perm, key_sign = jax.random.split(key, 4)
    devices = IMAGES // IMG_DEV
    row_device = jnp.arange(IMAGES) // IMG_DEV
    target = jax.random.permutation(key_perm, devices)[row_device]
    boosted = jnp.arange(F)[None, :] % devices == target[:, None]
    signs = jnp.where(jax.random.randint(key_sign, (devices,), 0, 2) == 0, -1.0, 1.0)[row_device]
    offset = 0.5 * jnp.clip(jax.random.normal(key_offset, (F,)), -4.0, 4.0)
    noise = jnp.clip(jax.random.normal(key_noise, (IMAGES, F)), -4.0, 4.0)
    values = offset[None, :] + noise + 4.0 * signs[:, None] * boosted.astype(jnp.float32)
    return jnp.clip(values, -20.0, 20.0).astype(jnp.float32).astype(jnp.bfloat16)


def raised(drawn, own_key, source, target, blocks, factor):
    owner, partner = [(jnp.arange(drawn.shape[axis_at]) // (drawn.shape[axis_at] // blocks)).reshape([-1 if axis == axis_at else 1 for axis in range(drawn.ndim)]) for axis_at in (source, target)]
    chosen = jax.random.permutation(own_key, blocks)[partner]
    strong = (owner == chosen) | (owner == (partner + blocks // 2) % blocks)
    return jnp.where(strong, factor * drawn, drawn)


def shard_levels(key, shape, cuts, smallest, largest):
    level, own = 1.0, jax.random.fold_in(key, 6)
    for position, blocks in cuts:
        steps = jnp.exp(jax.random.uniform(jax.random.fold_in(own, position), (blocks,), jnp.float32, smallest / len(cuts), largest / len(cuts)))
        level = level * jnp.repeat(steps, shape[position] // blocks).reshape([-1 if axis == position else 1 for axis in range(len(shape))])
    return level


def bell_draw(rng, shape, deviation, most, shards=(), held_as=jnp.bfloat16):
    result = deviation * jax.random.normal(rng, shape, jnp.float32)
    if shards:
        result = result * shard_levels(rng, shape, shards, -0.22, 0.18)
    return jnp.clip(result, -most, most).astype(held_as)


def gaussian_with(key, dims, spread, bound, shards, heavy, held_as=jnp.bfloat16):
    entries = spread * jax.random.normal(key, dims, jnp.float32)
    if shards:
        entries = entries * shard_levels(key, dims, shards, -0.22, 0.18)
    return jnp.clip(raised(entries, jax.random.fold_in(key, 3), *heavy), -bound, bound).astype(held_as)


def setup_inputs(seed: int = 0) -> dict:
    key_list = jax.random.split(jax.random.key(seed), 8)
    pre_norm = bell_draw(key_list[0], (IMAGES, F), 1.0, 6.0, ((0, 32),))
    upstream = draw_upstream(jax.random.fold_in(key_list[7], 71), 0)
    norm_gain = jnp.clip(1.0 + 0.18 * jax.random.normal(key_list[2], (F,), jnp.float32), 0.1, 1.9)
    saved_mean = bell_draw(key_list[3], (F,), 0.3, 4.0, (), jnp.float32)
    inv_std = jnp.clip(jnp.exp(jax.random.uniform(key_list[4], (F,), jnp.float32, math.log(0.5), math.log(1.5))), 0.5, 1.5)
    features = gaussian_with(key_list[5], (IMAGES * SPATIAL, CIN), 1.0, 6.0, ((0, 32),), (0, 1, 32, 2.75))
    out_grads = bell_draw(key_list[6], (IMAGES * SPATIAL, COUT), 4.0, 24.0, ((0, 32),))
    return {"pre_norm": pre_norm, "upstream": upstream, "norm_gain": norm_gain, "saved_mean": saved_mean, "inv_std": inv_std, "features": features, "out_grads": out_grads}


def reference(pre_norm, upstream, norm_gain, saved_mean, inv_std, features, out_grads):
    normed = (pre_norm.astype(jnp.float32) - saved_mean) * inv_std
    grads32 = upstream.astype(jnp.float32)
    bias_grad = jnp.sum(grads32, axis=0) / IMAGES
    gain_grad = jnp.sum(grads32 * normed, axis=0) / IMAGES
    input_grad = (norm_gain * inv_std * (grads32 - bias_grad - normed * gain_grad)).astype(jnp.bfloat16)
    blocks = IMAGES // IMG_DEV
    feat_blocks = features.reshape(blocks, IMG_DEV * SPATIAL, CIN)
    grad_blocks = out_grads.reshape(blocks, IMG_DEV * SPATIAL, COUT)

    def accumulate(total, pair):
        left, right = pair
        product = jnp.dot(left.astype(jnp.float32).T, right.astype(jnp.float32), precision=lax.Precision.HIGHEST)
        return total + product, None

    total, unused = lax.scan(accumulate, jnp.zeros((CIN, COUT), jnp.float32), (feat_blocks, grad_blocks))
    weight_grad = total / IMAGES
    return input_grad, gain_grad, bias_grad, weight_grad
```

```python
import jax
import jax.numpy as jnp
from jax import lax
from jax.sharding import PartitionSpec as P


def log2(count):
    return count.bit_length() - 1


def swap(value, axis, bit):
    count = lax.axis_size(axis)
    return lax.ppermute(value, axis, [(i, i ^ (1 << bit)) for i in range(count)])


def my_bit(axis, bit):
    return (lax.axis_index(axis) >> bit) & 1


def halves(value, dim, chosen):
    keep = lax.dynamic_index_in_dim(value, chosen, dim, keepdims=False)
    send = lax.dynamic_index_in_dim(value, 1 - chosen, dim, keepdims=False)
    return keep, send


def owner_step(value, left_bits, bit):
    blocks, rows, cols = value.shape
    place = left_bits.index(bit)
    split = value.reshape(1 << place, 2, blocks >> (place + 1), rows, cols)
    keep, send = halves(split, 1, my_bit("zero", bit))
    total = keep + swap(send, "zero", bit)
    return total.reshape(blocks // 2, rows, cols)


def column_step(value, bit):
    blocks, rows, cols = value.shape
    start = my_bit("rep", bit) * (cols // 2)
    other = (1 - my_bit("rep", bit)) * (cols // 2)
    keep = lax.dynamic_slice_in_dim(value, start, cols // 2, 2)
    send = lax.dynamic_slice_in_dim(value, other, cols // 2, 2)
    return keep + swap(send, "rep", bit)


def join_step(value, bit):
    rows, cols = value.shape
    got = swap(value, "rep", bit)
    mine = my_bit("rep", bit) == 0
    return jnp.concatenate((jnp.where(mine, value, got), jnp.where(mine, got, value)), axis=1)


def all_sum(value):
    for bit in range(log2(lax.axis_size("zero"))):
        value = value + swap(value, "zero", bit)
    for bit in range(log2(lax.axis_size("rep"))):
        value = value + swap(value, "rep", bit)
    return value


def chunk_sum(partial, rep_bits):
    owner_bits = list(range(log2(lax.axis_size("zero"))))
    left = owner_bits[::-1]
    value = owner_step(partial, left, 0)
    left.remove(0)
    for bit in rep_bits:
        value = column_step(value, bit)
    for bit in owner_bits[1:]:
        value = owner_step(value, left, bit)
        left.remove(bit)
    value = value[0]
    for bit in rep_bits[::-1]:
        value = join_step(value, bit)
    return value


def per_device(pre_norm, upstream, norm_gain, saved_mean, inv_std, features, out_grads):
    num_rep = lax.axis_size("rep")
    num_zero = lax.axis_size("zero")
    all_images = pre_norm.shape[0] * num_rep * num_zero
    normed = (pre_norm.astype(jnp.float32) - saved_mean) * inv_std
    grads32 = upstream.astype(jnp.float32)
    local_sums = jnp.stack((jnp.sum(grads32, axis=0), jnp.sum(grads32 * normed, axis=0)))
    stacked_sums = all_sum(local_sums)
    bias_grad = stacked_sums[0] / all_images
    gain_grad = stacked_sums[1] / all_images
    input_grad = (norm_gain * inv_std * (grads32 - bias_grad - normed * gain_grad)).astype(
        jnp.bfloat16
    )
    cin, cout = features.shape[1], out_grads.shape[1]
    rep_bits = list(range(log2(num_rep)))
    pieces = []
    chunks = 2
    for chunk in range(chunks):
        wide = cout // chunks
        partial_grad = lax.dot_general(
            features,
            out_grads[:, chunk * wide : (chunk + 1) * wide],
            (((0,), (0,)), ((), ())),
            preferred_element_type=jnp.float32,
        )
        blocks = partial_grad.reshape(num_zero, cin // num_zero, wide)
        pieces.append(chunk_sum(blocks, rep_bits if chunk % 2 == 0 else rep_bits[::-1]))
    weight_grad = jnp.concatenate(pieces, axis=1) / all_images
    return (input_grad, gain_grad, bias_grad, weight_grad)


def solution(mesh):
    return jax.shard_map(
        per_device,
        mesh=mesh,
        in_specs=(
            P(("rep", "zero"), None),
            P(("rep", "zero"), None),
            P(),
            P(),
            P(),
            P(("rep", "zero"), None),
            P(("rep", "zero"), None),
        ),
        out_specs=(P(("rep", "zero"), None), P(), P(), P("zero", None)),
        check_vma=False,
    )
```

```python
import jax
import jax.numpy as jnp
from jax import lax
from jax.sharding import PartitionSpec as P


def log2(count):
    return count.bit_length() - 1


def swap(value, axis, mask):
    count = lax.axis_size(axis)
    return lax.ppermute(value, axis, [(i, i ^ mask) for i in range(count)])


def my_bit(axis, bit):
    return (lax.axis_index(axis) >> bit) & 1


def owner_step(value, left_bits, bit):
    blocks, rows, cols = value.shape
    place = left_bits.index(bit)
    split = value.reshape(1 << place, 2, blocks >> (place + 1), rows, cols)
    mine = my_bit("zero", bit)
    keep = lax.dynamic_index_in_dim(split, mine, 1, keepdims=False)
    send = lax.dynamic_index_in_dim(split, 1 - mine, 1, keepdims=False)
    total = keep + swap(send, "zero", 1 << bit)
    left_bits.remove(bit)
    return total.reshape(blocks // 2, rows, cols)


def column_step(value, bit):
    half = value.shape[2] // 2
    mine = my_bit("rep", bit)
    keep = lax.dynamic_slice_in_dim(value, mine * half, half, 2)
    send = lax.dynamic_slice_in_dim(value, (1 - mine) * half, half, 2)
    return keep + swap(send, "rep", 1 << bit)


def join(pieces, orders):
    count = len(orders[0])
    stop = count
    while stop > 0:
        start = (stop - 1) // 2 * 2
        stacked = jnp.stack(pieces)
        span = stop - start
        group = sorted(orders[0][start:stop])
        got = {}
        for local in range(1 << span):
            mask = sum(((local >> k) & 1) << bit for k, bit in enumerate(group))
            got[mask] = stacked if mask == 0 else swap(stacked, "rep", mask)
        joined = []
        for chunk, order in enumerate(orders):
            bits = order[start:stop]
            mine = 0
            for bit in bits:
                mine = mine * 2 + my_bit("rep", bit)
            choices = []
            for local in range(1 << span):
                mask = sum(((local >> (span - 1 - k)) & 1) << bit for k, bit in enumerate(bits))
                choices.append(got[mask][chunk])
            slots = []
            for slot in range(1 << span):
                picked = choices[0]
                for local in range(1, 1 << span):
                    picked = jnp.where((mine ^ slot) == local, choices[local], picked)
                slots.append(picked)
            joined.append(jnp.concatenate(slots, axis=1))
        pieces = joined
        stop = start
    return pieces


def dot(left, right):
    return lax.dot_general(
        left, right, (((0,), (0,)), ((), ())), preferred_element_type=jnp.float32
    )


def per_device(pre_norm, upstream, norm_gain, saved_mean, inv_std, features, out_grads):
    num_rep = lax.axis_size("rep")
    num_zero = lax.axis_size("zero")
    all_images = pre_norm.shape[0] * num_rep * num_zero
    depth, cin = features.shape
    cout = out_grads.shape[1]
    rows = cin // num_zero
    owner_bits = list(range(log2(num_zero)))
    rep_bits = list(range(log2(num_rep)))
    swapped = [bit ^ 1 if bit ^ 1 < len(rep_bits) else bit for bit in rep_bits]
    orders = [rep_bits, swapped]
    wide = cout // 2
    half = wide // 2

    core = my_bit("zero", 0)
    parts = features.reshape(depth, num_zero // 2, 2, rows)
    send_feat = lax.dynamic_index_in_dim(parts, 1 - core, 2, keepdims=False).reshape(depth, -1)
    keep_feat = lax.dynamic_index_in_dim(parts, core, 2, keepdims=False).reshape(depth, -1)
    first = [my_bit("rep", order[0]) for order in orders]
    leave = [
        lax.dynamic_slice_in_dim(out_grads, chunk * wide + (1 - first[chunk]) * half, half, 1)
        for chunk in range(2)
    ]
    stay = [
        lax.dynamic_slice_in_dim(out_grads, chunk * wide + first[chunk] * half, half, 1)
        for chunk in range(2)
    ]
    leave_other = swap(dot(send_feat, jnp.concatenate(leave, axis=1)), "zero", 1)
    stay_other = swap(dot(send_feat, jnp.concatenate(stay, axis=1)), "zero", 1)
    leaving = [
        dot(keep_feat, leave[chunk]) + leave_other[:, chunk * half : (chunk + 1) * half]
        for chunk in range(2)
    ]

    normed = (pre_norm.astype(jnp.float32) - saved_mean) * inv_std
    grads32 = upstream.astype(jnp.float32)
    sums = jnp.stack((jnp.sum(grads32, axis=0), jnp.sum(grads32 * normed, axis=0)))
    leaving[0], leaving[1], sums = lax.optimization_barrier((leaving[0], leaving[1], sums))
    arrived = [swap(leaving[chunk], "rep", 1 << orders[chunk][0]) for chunk in range(2)]
    for bit in owner_bits:
        sums = sums + swap(sums, "zero", 1 << bit)

    values = []
    for chunk in range(2):
        staying = dot(keep_feat, stay[chunk]) + stay_other[:, chunk * half : (chunk + 1) * half]
        values.append((staying + arrived[chunk]).reshape(num_zero // 2, rows, half))
    values[0], values[1], sums = lax.optimization_barrier((values[0], values[1], sums))
    for step in range(1, len(rep_bits)):
        values = [column_step(values[chunk], orders[chunk][step]) for chunk in range(2)]
    for bit in rep_bits:
        sums = sums + swap(sums, "rep", 1 << bit)
    left = [owner_bits[:0:-1], owner_bits[:0:-1]]
    for step in range(1, len(owner_bits)):
        values = [
            owner_step(values[0], left[0], owner_bits[step]),
            owner_step(values[1], left[1], owner_bits[len(owner_bits) - step]),
        ]
    pieces = join([value[0] / all_images for value in values], orders)
    weight_grad = jnp.concatenate(pieces, axis=1)

    bias_grad = sums[0] / all_images
    gain_grad = sums[1] / all_images
    input_grad = (norm_gain * inv_std * (grads32 - bias_grad - normed * gain_grad)).astype(
        jnp.bfloat16
    )
    return (input_grad, gain_grad, bias_grad, weight_grad)


def solution(mesh):
    return jax.shard_map(
        per_device,
        mesh=mesh,
        in_specs=(
            P(("rep", "zero"), None),
            P(("rep", "zero"), None),
            P(),
            P(),
            P(),
            P(("rep", "zero"), None),
            P(("rep", "zero"), None),
        ),
        out_specs=(P(("rep", "zero"), None), P(), P(), P("zero", None)),
        check_vma=False,
    )
```

```python
import jax
import jax.numpy as jnp
from jax import lax
from jax.sharding import PartitionSpec as P


def log2(count):
    return count.bit_length() - 1


def swap(value, axis, mask):
    count = lax.axis_size(axis)
    return lax.ppermute(value, axis, [(i, i ^ mask) for i in range(count)])


def my_bit(axis, bit):
    return (lax.axis_index(axis) >> bit) & 1


def owner_cut(value, left_bits, bit):
    blocks, rows, cols = value.shape
    place = left_bits.index(bit)
    left_bits.remove(bit)
    split = value.reshape(1 << place, 2, blocks >> (place + 1), rows, cols)
    mine = my_bit("zero", bit)
    keep = lax.dynamic_index_in_dim(split, mine, 1, keepdims=False)
    send = lax.dynamic_index_in_dim(split, 1 - mine, 1, keepdims=False)
    return keep.reshape(blocks // 2, rows, cols), send.reshape(blocks // 2, rows, cols)


def column_cut(value, bit):
    half = value.shape[2] // 2
    mine = my_bit("rep", bit)
    keep = lax.dynamic_slice_in_dim(value, mine * half, half, 2)
    send = lax.dynamic_slice_in_dim(value, (1 - mine) * half, half, 2)
    return keep, send


def join(pieces, orders):
    count = len(orders[0])
    stop = count
    while stop > 0:
        start = (stop - 1) // 2 * 2
        stacked = jnp.stack(pieces)
        span = stop - start
        group = sorted(orders[0][start:stop])
        got = {}
        for local in range(1 << span):
            mask = sum(((local >> k) & 1) << bit for k, bit in enumerate(group))
            got[mask] = stacked if mask == 0 else swap(stacked, "rep", mask)
        joined = []
        for chunk, order in enumerate(orders):
            bits = order[start:stop]
            mine = 0
            for bit in bits:
                mine = mine * 2 + my_bit("rep", bit)
            choices = []
            for local in range(1 << span):
                mask = sum(((local >> (span - 1 - k)) & 1) << bit for k, bit in enumerate(bits))
                choices.append(got[mask][chunk])
            slots = []
            for slot in range(1 << span):
                picked = choices[0]
                for local in range(1, 1 << span):
                    picked = jnp.where((mine ^ slot) == local, choices[local], picked)
                slots.append(picked)
            joined.append(jnp.concatenate(slots, axis=1))
        pieces = joined
        stop = start
    return pieces


def dot(left, right):
    return lax.dot_general(
        left, right, (((0,), (0,)), ((), ())), preferred_element_type=jnp.float32
    )


def per_device(pre_norm, upstream, norm_gain, saved_mean, inv_std, features, out_grads):
    num_rep = lax.axis_size("rep")
    num_zero = lax.axis_size("zero")
    all_images = pre_norm.shape[0] * num_rep * num_zero
    depth, cin = features.shape
    cout = out_grads.shape[1]
    rows = cin // num_zero
    owner_bits = list(range(log2(num_zero)))
    rep_bits = list(range(log2(num_rep)))
    swapped = [bit ^ 1 if bit ^ 1 < len(rep_bits) else bit for bit in rep_bits]
    orders = [rep_bits, swapped]
    wide = cout // 2
    half = wide // 2

    core = my_bit("zero", 0)
    parts = features.reshape(depth, num_zero // 2, 2, rows)
    send_feat = lax.dynamic_index_in_dim(parts, 1 - core, 2, keepdims=False).reshape(depth, -1)
    keep_feat = lax.dynamic_index_in_dim(parts, core, 2, keepdims=False).reshape(depth, -1)
    first = [my_bit("rep", order[0]) for order in orders]
    leave = [
        lax.dynamic_slice_in_dim(out_grads, chunk * wide + (1 - first[chunk]) * half, half, 1)
        for chunk in range(2)
    ]
    stay = [
        lax.dynamic_slice_in_dim(out_grads, chunk * wide + first[chunk] * half, half, 1)
        for chunk in range(2)
    ]
    leave_other = swap(dot(send_feat, jnp.concatenate(leave, axis=1)), "zero", 1)
    stay_other = swap(dot(send_feat, jnp.concatenate(stay, axis=1)), "zero", 1)
    leaving = [
        dot(keep_feat, leave[chunk]) + leave_other[:, chunk * half : (chunk + 1) * half]
        for chunk in range(2)
    ]

    normed = (pre_norm.astype(jnp.float32) - saved_mean) * inv_std
    grads32 = upstream.astype(jnp.float32)
    sums = jnp.stack((jnp.sum(grads32, axis=0), jnp.sum(grads32 * normed, axis=0)))
    sums = sums + swap(sums, "zero", 1)
    leaving[1], sums = lax.optimization_barrier((leaving[1], sums))
    arrived = [swap(leaving[chunk], "rep", 1 << orders[chunk][0]) for chunk in range(2)]
    for bit in owner_bits[1:]:
        sums = sums + swap(sums, "zero", 1 << bit)

    values = []
    for chunk in range(2):
        staying = dot(keep_feat, stay[chunk]) + stay_other[:, chunk * half : (chunk + 1) * half]
        values.append((staying + arrived[chunk]).reshape(num_zero // 2, rows, half))

    left = [owner_bits[:0:-1], owner_bits[:0:-1]]
    waiting = list(rep_bits)
    phases = [("rep", [order[step] for order in orders]) for step in range(1, len(rep_bits))]
    for step in range(1, len(owner_bits)):
        phases.append(("zero", [owner_bits[step], owner_bits[len(owner_bits) - step]]))
    for axis, bits in phases:
        pairs = []
        for chunk in range(2):
            if axis == "rep":
                pairs.append(column_cut(values[chunk], bits[chunk]))
            else:
                pairs.append(owner_cut(values[chunk], left[chunk], bits[chunk]))
        keeps = [pair[0] for pair in pairs]
        sends = [pair[1] for pair in pairs]
        if waiting:
            sends[1], sums = lax.optimization_barrier((sends[1], sums))
        values = [
            keeps[chunk] + swap(sends[chunk], axis, 1 << bits[chunk]) for chunk in range(2)
        ]
        if waiting:
            sums = sums + swap(sums, "rep", 1 << waiting.pop(0))
    for bit in waiting:
        sums = sums + swap(sums, "rep", 1 << bit)
    pieces = join([value[0] / all_images for value in values], orders)
    weight_grad = jnp.concatenate(pieces, axis=1)

    bias_grad = sums[0] / all_images
    gain_grad = sums[1] / all_images
    input_grad = (norm_gain * inv_std * (grads32 - bias_grad - normed * gain_grad)).astype(
        jnp.bfloat16
    )
    return (input_grad, gain_grad, bias_grad, weight_grad)


def solution(mesh):
    return jax.shard_map(
        per_device,
        mesh=mesh,
        in_specs=(
            P(("rep", "zero"), None),
            P(("rep", "zero"), None),
            P(),
            P(),
            P(),
            P(("rep", "zero"), None),
            P(("rep", "zero"), None),
        ),
        out_specs=(P(("rep", "zero"), None), P(), P(), P("zero", None)),
        check_vma=False,
    )
```
